32 devices in a mesh: row: 4 (over y, core), col: 8 (over z, x).
Axes of the slice: x: 2, y: 2, z: 4, core: 2. Of those that a mesh axis runs over, the one named last changes fastest.
Arguments:
- first_acts: bfloat16 [2048, 18944], P('col', 'row'), may hold values from -320 to 320, as said below
- second_acts: bfloat16 [2048, 18944], P('row', 'col'), may hold values from -320 to 320, as said below
Outputs:
- row_potential: float32 [18944], P('row')
- column_potential: float32 [18944], P('col')
The draws below stay inside these ranges and needn't reach their ends.
Inputs may be any that keep to these rules, and one draw needn't show every extreme that they name: `first_acts`: real-valued activations. `second_acts`: real-valued activations.
All inputs are finite; a program needn't handle non-finite values.
Results may differ from the reference program's by a relative error of at most 0.0003.
Values may be sent and summed in bfloat16 or wider, within the bound.
A program may use at most 128 MiB of HBM per device.

```python
import math
import jax
import jax.numpy as jnp
from jax import lax

NEUR = 18944
SAMP = 2048
ITERS = 4
N_ROW = 4


def activation_pair(key):
    keys = jax.random.split(jax.random.fold_in(key, 91), 4)
    first = jnp.clip(jax.random.normal(keys[0], (SAMP, NEUR), jnp.float32), -6.0, 6.0)
    second = jnp.clip(jax.random.normal(keys[1], (SAMP, NEUR), jnp.float32), -6.0, 6.0)
    scale_first = jnp.exp(jax.random.uniform(keys[2], (NEUR,), jnp.float32, 0.0, math.log(10.0)))
    scale_second = jnp.exp(jax.random.uniform(keys[3], (NEUR,), jnp.float32, 0.0, math.log(10.0)))
    return (first * scale_first[None, :], second * scale_second[None, :])


def draw_first_acts(key, part):
    return activation_pair(key)[0].astype(jnp.bfloat16)


def draw_second_acts(key, part):
    return activation_pair(key)[1].astype(jnp.bfloat16)


def setup_inputs(seed: int = 0) -> dict:
    seeds = jax.random.split(jax.random.key(seed), 3)
    return {
        "first_acts": draw_first_acts(jax.random.fold_in(seeds[2], 71), 0),
        "second_acts": draw_second_acts(jax.random.fold_in(seeds[2], 71), 0),
    }


entropy_scale = 0.004

def reference(first_acts, second_acts):
    first_wide = first_acts.astype(jnp.float32)
    second_wide = second_acts.astype(jnp.float32)
    inv_first = 1.0 / jnp.sqrt(lax.optimization_barrier(jnp.sum(first_wide * first_wide, 0)) / SAMP + 1e-06)
    inv_second = 1.0 / jnp.sqrt(lax.optimization_barrier(jnp.sum(second_wide * second_wide, 0)) / SAMP + 1e-06)
    products = jnp.dot(first_acts.T, second_acts, preferred_element_type=jnp.float32)
    logk = products * inv_first[:, None] * inv_second[None, :] * (1.0 / (SAMP * entropy_scale))
    block_rows = NEUR // N_ROW
    blocks = logk.reshape(N_ROW, block_rows, NEUR)
    log_share = -math.log(NEUR)
    row_potential = jnp.zeros((NEUR,), jnp.float32)
    column_potential = jnp.zeros((NEUR,), jnp.float32)
    for step in range(ITERS):

        def row_lse(block):
            scores = column_potential[None, :] + block
            highest = lax.optimization_barrier(jnp.max(scores, 1))
            return highest + jnp.log(lax.optimization_barrier(jnp.sum(jnp.exp(scores - highest[:, None]), 1)))
        row_potential = log_share - lax.map(row_lse, blocks).reshape(NEUR)
        row_blocks = row_potential.reshape(N_ROW, block_rows)

        def col_step(running, element):
            run_max, run_sum = running
            block, potentials = element
            scores = potentials[:, None] + block
            highest = jnp.maximum(run_max, lax.optimization_barrier(jnp.max(scores, 0)))
            run_sum = run_sum * jnp.exp(run_max - highest) + lax.optimization_barrier(jnp.sum(jnp.exp(scores - highest[None, :]), 0))
            return ((highest, run_sum), None)
        start_max = jnp.full((NEUR,), -1e+30, jnp.float32)
        start_sum = jnp.zeros((NEUR,), jnp.float32)
        (col_max, col_sum), unused = lax.scan(col_step, (start_max, start_sum), (blocks, row_blocks))
        column_potential = log_share - (col_max + jnp.log(col_sum))
    return (row_potential, column_potential)
```

```python
import functools
import math

import jax
import jax.numpy as jnp
from jax import lax
from jax.experimental import pallas as pl
from jax.experimental.pallas import tpu as pltpu
from jax.sharding import PartitionSpec as P

ITERS = 4
ENTROPY_SCALE = 0.004
LOG2E = 1.0 / math.log(2.0)
LN2 = math.log(2.0)
SHIFT = 58.0
LOW = -1e30
LANES = 128
MESH = pl.DeviceIdType.MESH


def round_up(value, unit):
    return -(-value // unit) * unit


def kernel(
    rows, cols, total, samples,
    a_hbm, b_ref, row_out, col_out,
    acc, abuf, f_vec, g_vec, a_vec, b_vec, inv_b, col_max, col_sum,
    send_r0, recv_r0, send_r, recv_r, send_c0, recv_c0, send_c, recv_c,
    load_sem, rs0, rr0, rs, rr, cs0, cr0, cs, cr,
):
    n_row, n_col = lax.axis_size("row"), lax.axis_size("col")
    my_row, my_col = lax.axis_index("row"), lax.axis_index("col")
    chunks, rows_pad, depth = a_hbm.shape
    cols_pad = b_ref.shape[1]
    tile = abuf.shape[1]
    share = -math.log(total) * LOG2E
    blocks = rows_pad // LANES
    lane_tiles = cols_pad // LANES

    barrier = pltpu.get_barrier_semaphore()
    for axis, me, n in (("row", my_row, n_row), ("col", my_col, n_col)):
        for d in range(1, n):
            pl.semaphore_signal(
                barrier, inc=1, device_id={axis: lax.rem(me + d, n)}, device_id_type=MESH
            )
    pl.semaphore_wait(barrier, n_row + n_col - 2)

    def exchange(axis, me, n, send, recv, ssem, rsem):
        copies = []
        for d in range(1, n):
            copy = pltpu.make_async_remote_copy(
                src_ref=send,
                dst_ref=recv.at[d - 1],
                send_sem=ssem.at[d - 1],
                recv_sem=rsem.at[d - 1],
                device_id={axis: lax.rem(me + d, n)},
                device_id_type=MESH,
            )
            copy.start()
            copies.append(copy)
        for copy in copies:
            copy.wait()

    def load(index, start, size, slot):
        return [
            pltpu.make_async_copy(
                a_hbm.at[c, pl.ds(start, size), :],
                abuf.at[slot, pl.ds(0, size), pl.ds(c * depth, depth)],
                load_sem.at[slot, c],
            )
            for c in range(chunks)
        ]

    full = rows_pad // tile
    tail = rows_pad - full * tile

    if full:
        for copy in load(0, 0, tile, 0):
            copy.start()

    def square_step(i, unused):
        part = b_ref[pl.ds(pl.multiple_of(i * 32, 32), 32), :].astype(jnp.float32)
        sq = part * part
        col_sum[...] += sq[0:8] + sq[8:16] + sq[16:24] + sq[24:32]
        return unused

    col_sum[...] = jnp.zeros_like(col_sum)
    lax.fori_loop(0, samples // 32, square_step, 0)
    sq_b = jnp.sum(col_sum[...], 0, keepdims=True)
    inv_b[...] = (LOG2E / (samples * ENTROPY_SCALE)) / jnp.sqrt(sq_b / samples + 1e-6)

    n_tile = 1024
    n_edges = [(s, min(s + n_tile, cols_pad)) for s in range(0, cols_pad, n_tile)]

    def matmul_tile(start, size, slot):
        a_tile = abuf.at[slot]
        sq = jnp.zeros((size, LANES), jnp.float32)
        for k in range(samples // LANES):
            w = a_tile[0:size, k * LANES:(k + 1) * LANES].astype(jnp.float32)
            sq = sq + w * w
        inv_a = 1.0 / jnp.sqrt(jnp.sum(sq, 1, keepdims=True) / samples + 1e-6)
        for lo, hi in n_edges:
            prod = jnp.dot(
                a_tile[0:size, :], b_ref[:, lo:hi], preferred_element_type=jnp.float32
            )
            x = prod * inv_a * inv_b[:, lo:hi]
            if hi > cols:
                lane = lax.broadcasted_iota(jnp.int32, (size, hi - lo), 1) + lo
                x = jnp.where(lane < cols, x, LOW)
            acc[pl.ds(start, size), lo:hi] = x

    def row_stats(i, unused):
        at = pl.ds(pl.multiple_of(i * LANES, LANES), LANES)
        top = acc[at, 0:LANES]
        for k in range(1, lane_tiles):
            top = jnp.maximum(top, acc[at, k * LANES:(k + 1) * LANES])
        top = jnp.broadcast_to(jnp.max(top, 1, keepdims=True), (LANES, LANES))
        part = jnp.zeros((LANES, LANES), jnp.float32)
        for k in range(lane_tiles):
            part = part + jnp.exp2(acc[at, k * LANES:(k + 1) * LANES] - top)
        send_r0[0:1, at] = top.T[0:1]
        send_r0[1:2, at] = jnp.sum(part.T, 0, keepdims=True)
        return unused

    def tile_step(t, unused):
        slot = lax.rem(t, 2)
        start = pl.multiple_of(t * tile, tile)
        for copy in load(t, start, tile, slot):
            copy.wait()

        @pl.when(t + 1 < full)
        def _():
            for copy in load(t + 1, pl.multiple_of((t + 1) * tile, tile), tile, 1 - slot):
                copy.start()

        matmul_tile(start, tile, slot)
        lax.fori_loop(t * (tile // LANES), (t + 1) * (tile // LANES), row_stats, 0)
        return unused

    if full:
        lax.fori_loop(0, full, tile_step, 0)
    if tail:
        slot = full % 2
        copies = load(full, full * tile, tail, slot)
        for copy in copies:
            copy.start()
        for copy in copies:
            copy.wait()
        matmul_tile(full * tile, tail, slot)
        lax.fori_loop(full * (tile // LANES), blocks, row_stats, 0)

    def merge(send, recv, n):
        parts = [send[...]] + [recv[d] for d in range(n - 1)]
        top = parts[0][0:1]
        for p in parts[1:]:
            top = jnp.maximum(top, p[0:1])
        acc_sum = jnp.zeros_like(top)
        for p in parts:
            acc_sum = acc_sum + p[1:2] * jnp.exp2(p[0:1] - top)
        return share - (top + jnp.log(acc_sum) * LOG2E)

    exchange("col", my_col, n_col, send_r0, recv_r0, rs0, rr0)
    first_f = merge(send_r0, recv_r0, n_col)
    if rows_pad != rows:
        first_f = jnp.where(
            lax.broadcasted_iota(jnp.int32, (1, rows_pad), 1) < rows, first_f, LOW
        )
    f_vec[...] = first_f

    def spread(ref, at):
        return jnp.broadcast_to(ref[:, at], (LANES, LANES)).T

    def fold(value, op):
        parts = [value[8 * s:8 * s + 8] for s in range(value.shape[0] // 8)]
        while len(parts) > 1:
            parts = [op(parts[i], parts[i + 1]) for i in range(0, len(parts), 2)]
        return parts[0]

    col_max[...] = jnp.full(col_max.shape, 2 * LOW, jnp.float32)
    col_sum[...] = jnp.zeros_like(col_sum)

    def first_col(i, unused):
        at = pl.ds(pl.multiple_of(i * LANES, LANES), LANES)
        f_rep = spread(f_vec, at)
        for k in range(lane_tiles):
            lanes = slice(k * LANES, (k + 1) * LANES)
            y = acc[at, lanes] + f_rep
            old = col_max[:, lanes]
            new = jnp.maximum(old, fold(y, jnp.maximum))
            e = jnp.exp2(y - jnp.concatenate([new] * (LANES // 8), 0))
            col_sum[:, lanes] = col_sum[:, lanes] * jnp.exp2(old - new) + fold(e, jnp.add)
            col_max[:, lanes] = new
        return unused

    lax.fori_loop(0, blocks, first_col, 0)
    top = jnp.max(col_max[...], 0, keepdims=True)
    send_c0[0:1, :] = top
    send_c0[1:2, :] = jnp.sum(col_sum[...] * jnp.exp2(col_max[...] - top), 0, keepdims=True)
    exchange("row", my_row, n_row, send_c0, recv_c0, cs0, cr0)
    first_g = merge(send_c0, recv_c0, n_row)
    if cols_pad != cols:
        first_g = jnp.where(
            lax.broadcasted_iota(jnp.int32, (1, cols_pad), 1) < cols, first_g, 0.0
        )
    g_vec[...] = first_g

    gain = 2.0 ** SHIFT / total

    for step in range(ITERS - 1):

        def row_pass(i, unused):
            at = pl.ds(pl.multiple_of(i * LANES, LANES), LANES)
            part = jnp.zeros((LANES, LANES), jnp.float32)
            if step == 0:
                f_rep = spread(f_vec, at) + SHIFT
            for k in range(lane_tiles):
                lanes = slice(k * LANES, (k + 1) * LANES)
                if step == 0:
                    p = jnp.exp2(acc[at, lanes] + f_rep + g_vec[:, lanes])
                    acc[at, lanes] = p
                    part = part + p
                else:
                    part = part + acc[at, lanes] * b_vec[:, lanes]
            send_r[step, 0:1, at] = jnp.sum(part.T, 0, keepdims=True)
            return unused

        lax.fori_loop(0, blocks, row_pass, 0)
        exchange("col", my_col, n_col, send_r.at[step], recv_r.at[step], rs.at[step], rr.at[step])
        merged = send_r[step]
        for d in range(n_col - 1):
            merged = merged + recv_r[step, d]
        scale_a = gain / merged
        if rows_pad != rows:
            scale_a = jnp.where(
                lax.broadcasted_iota(jnp.int32, (1, rows_pad), 1) < rows, scale_a, 0.0
            )
        a_vec[...] = scale_a
        col_sum[...] = jnp.zeros_like(col_sum)

        def col_pass(i, unused):
            at = pl.ds(pl.multiple_of(i * LANES, LANES), LANES)
            a_rep = spread(a_vec, at)
            for k in range(lane_tiles):
                lanes = slice(k * LANES, (k + 1) * LANES)
                col_sum[:, lanes] += fold(acc[at, lanes] * a_rep, jnp.add)
            return unused

        lax.fori_loop(0, blocks, col_pass, 0)
        send_c[step] = jnp.sum(col_sum[...], 0, keepdims=True)
        exchange("row", my_row, n_row, send_c.at[step], recv_c.at[step], cs.at[step], cr.at[step])
        merged = send_c[step]
        for d in range(n_row - 1):
            merged = merged + recv_c[step, d]
        scale_b = gain / merged
        if cols_pad != cols:
            scale_b = jnp.where(
                lax.broadcasted_iota(jnp.int32, (1, cols_pad), 1) < cols, scale_b, 1.0
            )
        b_vec[...] = scale_b

    row_out[...] = f_vec[...] * LN2 + jnp.log(a_vec[...])
    col_out[...] = g_vec[...] * LN2 + jnp.log(b_vec[...])


def shards(first_acts, second_acts):
    rows, cols = first_acts.shape[1], second_acts.shape[1]
    n_row, n_col = lax.axis_size("row"), lax.axis_size("col")
    samples = second_acts.shape[0] * n_row
    rows_pad, cols_pad = round_up(rows, LANES), round_up(cols, LANES)
    first = jnp.pad(first_acts, ((0, 0), (0, rows_pad - rows)))
    second = jnp.pad(second_acts, ((0, 0), (0, cols_pad - cols)))
    b_full = lax.all_gather(second, "row", axis=0, tiled=True)
    if first.shape[0] % LANES == 0:
        a_full = lax.all_gather(first.T, "col", axis=0, tiled=False)
    else:
        a_full = lax.all_gather(first, "col", axis=0, tiled=True).T[None]
    chunks = a_full.shape[0]
    tile = 512
    rest = ITERS - 1
    f32 = jnp.float32
    vmem = pltpu.VMEM
    dma = pltpu.SemaphoreType.DMA
    row_out, col_out = pl.pallas_call(
        functools.partial(kernel, rows, cols, rows * n_row, samples),
        out_shape=(
            jax.ShapeDtypeStruct((1, rows_pad), f32),
            jax.ShapeDtypeStruct((1, cols_pad), f32),
        ),
        in_specs=[pl.BlockSpec(memory_space=pl.ANY), pl.BlockSpec(memory_space=vmem)],
        out_specs=(pl.BlockSpec(memory_space=vmem),) * 2,
        scratch_shapes=[
            vmem((rows_pad, cols_pad), f32),
            vmem((2, tile, samples), jnp.bfloat16),
            vmem((1, rows_pad), f32),
            vmem((1, cols_pad), f32),
            vmem((1, rows_pad), f32),
            vmem((1, cols_pad), f32),
            vmem((1, cols_pad), f32),
            vmem((8, cols_pad), f32),
            vmem((8, cols_pad), f32),
            vmem((2, rows_pad), f32),
            vmem((n_col - 1, 2, rows_pad), f32),
            vmem((rest, 1, rows_pad), f32),
            vmem((rest, n_col - 1, 1, rows_pad), f32),
            vmem((2, cols_pad), f32),
            vmem((n_row - 1, 2, cols_pad), f32),
            vmem((rest, 1, cols_pad), f32),
            vmem((rest, n_row - 1, 1, cols_pad), f32),
            dma((2, chunks)),
            dma((n_col - 1,)),
            dma((n_col - 1,)),
            dma((rest, n_col - 1)),
            dma((rest, n_col - 1)),
            dma((n_row - 1,)),
            dma((n_row - 1,)),
            dma((rest, n_row - 1)),
            dma((rest, n_row - 1)),
        ],
        compiler_params=pltpu.CompilerParams(
            collective_id=0, has_side_effects=True, vmem_limit_bytes=67043328
        ),
    )(a_full, b_full)
    return row_out[0, :rows], col_out[0, :cols]


def solution(mesh):
    return jax.shard_map(
        shards,
        mesh=mesh,
        in_specs=(P("col", "row"), P("row", "col")),
        out_specs=(P("row"), P("col")),
        check_vma=False,
    )
```

```python
import functools
import math

import jax
import jax.numpy as jnp
from jax import lax
from jax.experimental import pallas as pl
from jax.experimental.pallas import tpu as pltpu
from jax.sharding import PartitionSpec as P

ITERS = 4
ENTROPY_SCALE = 0.004
LOG2E = 1.0 / math.log(2.0)
LN2 = math.log(2.0)
SHIFT = 58.0
LOW = -1e30
LANES = 128
MESH = pl.DeviceIdType.MESH


def round_up(value, unit):
    return -(-value // unit) * unit


def kernel(
    rows, cols, total, samples, tile, remote,
    a_hbm, b_hbm, row_out, col_out, a_full, b_ref,
    acc, abuf, f_vec, g_vec, a_vec, b_vec, inv_b, col_max, col_sum,
    send_r0, recv_r0, send_r, recv_r, send_c0, recv_c0, send_c, recv_c,
    load_sem, rs0, rr0, rs, rr, cs0, cr0, cs, cr,
    own_sem, ga_s, ga_r, gb_s, gb_r,
):
    n_row, n_col = lax.axis_size("row"), lax.axis_size("col")
    my_row, my_col = lax.axis_index("row"), lax.axis_index("col")
    rows_pad, depth = a_hbm.shape[1:]
    chunks = samples // depth
    cols_pad = b_ref.shape[1]
    b_depth = b_hbm.shape[0]
    share = -math.log(total) * LOG2E
    blocks = rows_pad // LANES
    lane_tiles = cols_pad // LANES

    barrier = pltpu.get_barrier_semaphore()
    for axis, me, n in (("row", my_row, n_row), ("col", my_col, n_col)):
        for d in range(1, n):
            pl.semaphore_signal(
                barrier, inc=1, device_id={axis: lax.rem(me + d, n)}, device_id_type=MESH
            )
    pl.semaphore_wait(barrier, n_row + n_col - 2)

    def exchange(axis, me, n, send, recv, ssem, rsem):
        copies = []
        for d in range(1, n):
            copy = pltpu.make_async_remote_copy(
                src_ref=send,
                dst_ref=recv.at[d - 1],
                send_sem=ssem.at[d - 1],
                recv_sem=rsem.at[d - 1],
                device_id={axis: lax.rem(me + d, n)},
                device_id_type=MESH,
            )
            copy.start()
            copies.append(copy)
        for copy in copies:
            copy.wait()

    full = rows_pad // tile
    tail = rows_pad - full * tile

    def relay(axis, me, n, src_of, dst_of, ssem, rsem):
        outer = n // 2
        mine_o, mine_i = me // 2, lax.rem(me, 2)

        def index(d, inner):
            return lax.rem(mine_o + d + outer, outer) * 2 + inner

        def copy(src, dst, slot, target):
            return pltpu.make_async_remote_copy(
                src_ref=src,
                dst_ref=dst,
                send_sem=ssem(slot),
                recv_sem=rsem(slot),
                device_id={axis: target},
                device_id_type=MESH,
            )

        partner = index(0, 1 - mine_i)
        own = [
            copy(src_of(), dst_of(me), d, index(d, mine_i)) for d in range(1, outer)
        ]
        own.append(copy(src_of(), dst_of(me), 0, partner))
        passed = []
        for d in range(1, outer):
            source = index(-d, mine_i)
            passed.append(copy(dst_of(source), dst_of(source), outer + d - 1, partner))
        return own, passed

    def a_relay(t, start, size):
        return relay(
            "col", my_col, n_col,
            lambda: a_hbm.at[0, pl.ds(start, size), :],
            lambda c: a_full.at[c, pl.ds(start, size), :],
            lambda k: ga_s.at[t, k],
            lambda k: ga_r.at[t, k],
        )

    def b_relay():
        return relay(
            "row", my_row, n_row,
            lambda: b_hbm,
            lambda c: b_ref.at[pl.ds(pl.multiple_of(c * b_depth, b_depth), b_depth), :],
            lambda k: gb_s.at[k],
            lambda k: gb_r.at[k],
        )

    def over_tiles(step):
        if full:
            lax.fori_loop(
                0, full, lambda t, u: (step(t, pl.multiple_of(t * tile, tile), tile), u)[1], 0
            )
        if tail:
            step(full, full * tile, tail)

    def send_tile(t, start, size):
        for copy in a_relay(t, start, size)[0]:
            copy.start()

    def pass_tile(t, start, size):
        own, passed = a_relay(t, start, size)
        for arrived, onward in zip(own, passed):
            arrived.wait_recv()
            onward.start()

    def wait_tile(t, start, size):
        own, passed = a_relay(t, start, size)
        own[-1].wait_recv()
        for copy in passed:
            copy.wait_recv()

    def close_tile(t, start, size):
        own, passed = a_relay(t, start, size)
        for copy in own + passed:
            copy.wait_send()

    if remote:
        base = pl.multiple_of(my_row * b_depth, b_depth)
    else:
        base = 0
    own_b = pltpu.make_async_copy(b_hbm, b_ref.at[pl.ds(base, b_depth), :], own_sem)
    own_b.start()
    if remote:
        b_own, b_passed = b_relay()
        for copy in b_own:
            copy.start()
        over_tiles(send_tile)
        for arrived, onward in zip(b_own, b_passed):
            arrived.wait_recv()
            onward.start()
        b_own[-1].wait_recv()
        for copy in b_passed:
            copy.wait_recv()
    own_b.wait()

    def load(start, size):
        copies = []
        for p in range(chunks):
            if remote:
                c = lax.rem(my_col + p, n_col)
                src = a_hbm.at[0] if p == 0 else a_full.at[c]
                lane = pl.multiple_of(c * depth, depth)
            else:
                src, lane = a_hbm.at[p], p * depth
            copies.append(
                pltpu.make_async_copy(
                    src.at[pl.ds(start, size), :],
                    abuf.at[pl.ds(0, size), pl.ds(lane, depth)],
                    load_sem.at[p],
                )
            )
        for copy in copies:
            copy.start()
        for copy in copies:
            copy.wait()

    def square_step(i, unused):
        part = b_ref[pl.ds(pl.multiple_of(i * 32, 32), 32), :].astype(jnp.float32)
        sq = part * part
        col_sum[...] += sq[0:8] + sq[8:16] + sq[16:24] + sq[24:32]
        return unused

    col_sum[...] = jnp.zeros_like(col_sum)
    lax.fori_loop(0, samples // 32, square_step, 0)
    sq_b = jnp.sum(col_sum[...], 0, keepdims=True)
    inv_b[...] = (LOG2E / (samples * ENTROPY_SCALE)) / jnp.sqrt(sq_b / samples + 1e-6)

    n_tile = 1024
    n_edges = [(s, min(s + n_tile, cols_pad)) for s in range(0, cols_pad, n_tile)]

    def matmul_tile(start, size):
        a_tile = abuf
        sq = jnp.zeros((size, LANES), jnp.float32)
        for k in range(samples // LANES):
            w = a_tile[0:size, k * LANES:(k + 1) * LANES].astype(jnp.float32)
            sq = sq + w * w
        inv_a = 1.0 / jnp.sqrt(jnp.sum(sq, 1, keepdims=True) / samples + 1e-6)
        for lo, hi in n_edges:
            prod = jnp.dot(
                a_tile[0:size, :], b_ref[:, lo:hi], preferred_element_type=jnp.float32
            )
            x = prod * inv_a * inv_b[:, lo:hi]
            if hi > cols:
                lane = lax.broadcasted_iota(jnp.int32, (size, hi - lo), 1) + lo
                x = jnp.where(lane < cols, x, LOW)
            acc[pl.ds(start, size), lo:hi] = x

    def row_stats(i, unused):
        at = pl.ds(pl.multiple_of(i * LANES, LANES), LANES)
        top = acc[at, 0:LANES]
        for k in range(1, lane_tiles):
            top = jnp.maximum(top, acc[at, k * LANES:(k + 1) * LANES])
        top = jnp.broadcast_to(jnp.max(top, 1, keepdims=True), (LANES, LANES))
        part = jnp.zeros((LANES, LANES), jnp.float32)
        for k in range(lane_tiles):
            part = part + jnp.exp2(acc[at, k * LANES:(k + 1) * LANES] - top)
        send_r0[0:1, at] = top.T[0:1]
        send_r0[1:2, at] = jnp.sum(part.T, 0, keepdims=True)
        return unused

    def compute(t, start, size):
        if remote:
            wait_tile(t, start, size)
        load(start, size)
        matmul_tile(start, size)
        first = t * (tile // LANES)
        lax.fori_loop(first, first + size // LANES, row_stats, 0)

    if remote:

        def tile_step(t, unused):
            pass_tile(t, pl.multiple_of(t * tile, tile), tile)

            @pl.when(t > 0)
            def _():
                compute(t - 1, pl.multiple_of((t - 1) * tile, tile), tile)

            return unused

        lax.fori_loop(0, full, tile_step, 0)
        if tail:
            pass_tile(full, full * tile, tail)
        compute(full - 1, (full - 1) * tile, tile)
        if tail:
            compute(full, full * tile, tail)
        for copy in b_own + b_passed:
            copy.wait_send()
        over_tiles(close_tile)
    else:
        over_tiles(compute)

    def merge(send, recv, n):
        parts = [send[...]] + [recv[d] for d in range(n - 1)]
        top = parts[0][0:1]
        for p in parts[1:]:
            top = jnp.maximum(top, p[0:1])
        acc_sum = jnp.zeros_like(top)
        for p in parts:
            acc_sum = acc_sum + p[1:2] * jnp.exp2(p[0:1] - top)
        return share - (top + jnp.log(acc_sum) * LOG2E)

    exchange("col", my_col, n_col, send_r0, recv_r0, rs0, rr0)
    first_f = merge(send_r0, recv_r0, n_col)
    if rows_pad != rows:
        first_f = jnp.where(
            lax.broadcasted_iota(jnp.int32, (1, rows_pad), 1) < rows, first_f, LOW
        )
    f_vec[...] = first_f

    def spread(ref, at):
        return jnp.broadcast_to(ref[:, at], (LANES, LANES)).T

    def fold(value, op):
        parts = [value[8 * s:8 * s + 8] for s in range(value.shape[0] // 8)]
        while len(parts) > 1:
            parts = [op(parts[i], parts[i + 1]) for i in range(0, len(parts), 2)]
        return parts[0]

    col_max[...] = jnp.full(col_max.shape, 2 * LOW, jnp.float32)
    col_sum[...] = jnp.zeros_like(col_sum)

    def first_col(i, unused):
        at = pl.ds(pl.multiple_of(i * LANES, LANES), LANES)
        f_rep = spread(f_vec, at)
        for k in range(lane_tiles):
            lanes = slice(k * LANES, (k + 1) * LANES)
            y = acc[at, lanes] + f_rep
            old = col_max[:, lanes]
            new = jnp.maximum(old, fold(y, jnp.maximum))
            e = jnp.exp2(y - jnp.concatenate([new] * (LANES // 8), 0))
            col_sum[:, lanes] = col_sum[:, lanes] * jnp.exp2(old - new) + fold(e, jnp.add)
            col_max[:, lanes] = new
        return unused

    lax.fori_loop(0, blocks, first_col, 0)
    top = jnp.max(col_max[...], 0, keepdims=True)
    send_c0[0:1, :] = top
    send_c0[1:2, :] = jnp.sum(col_sum[...] * jnp.exp2(col_max[...] - top), 0, keepdims=True)
    exchange("row", my_row, n_row, send_c0, recv_c0, cs0, cr0)
    first_g = merge(send_c0, recv_c0, n_row)
    if cols_pad != cols:
        first_g = jnp.where(
            lax.broadcasted_iota(jnp.int32, (1, cols_pad), 1) < cols, first_g, 0.0
        )
    g_vec[...] = first_g

    gain = 2.0 ** SHIFT / total

    for step in range(ITERS - 1):

        def row_pass(i, unused):
            at = pl.ds(pl.multiple_of(i * LANES, LANES), LANES)
            part = jnp.zeros((LANES, LANES), jnp.float32)
            if step == 0:
                f_rep = spread(f_vec, at) + SHIFT
            for k in range(lane_tiles):
                lanes = slice(k * LANES, (k + 1) * LANES)
                if step == 0:
                    p = jnp.exp2(acc[at, lanes] + f_rep + g_vec[:, lanes])
                    acc[at, lanes] = p
                    part = part + p
                else:
                    part = part + acc[at, lanes] * b_vec[:, lanes]
            send_r[step, 0:1, at] = jnp.sum(part.T, 0, keepdims=True)
            return unused

        lax.fori_loop(0, blocks, row_pass, 0)
        exchange("col", my_col, n_col, send_r.at[step], recv_r.at[step], rs.at[step], rr.at[step])
        merged = send_r[step]
        for d in range(n_col - 1):
            merged = merged + recv_r[step, d]
        scale_a = gain / merged
        if rows_pad != rows:
            scale_a = jnp.where(
                lax.broadcasted_iota(jnp.int32, (1, rows_pad), 1) < rows, scale_a, 0.0
            )
        a_vec[...] = scale_a
        col_sum[...] = jnp.zeros_like(col_sum)

        def col_pass(i, unused):
            at = pl.ds(pl.multiple_of(i * LANES, LANES), LANES)
            a_rep = spread(a_vec, at)
            for k in range(lane_tiles):
                lanes = slice(k * LANES, (k + 1) * LANES)
                col_sum[:, lanes] += fold(acc[at, lanes] * a_rep, jnp.add)
            return unused

        lax.fori_loop(0, blocks, col_pass, 0)
        send_c[step] = jnp.sum(col_sum[...], 0, keepdims=True)
        exchange("row", my_row, n_row, send_c.at[step], recv_c.at[step], cs.at[step], cr.at[step])
        merged = send_c[step]
        for d in range(n_row - 1):
            merged = merged + recv_c[step, d]
        scale_b = gain / merged
        if cols_pad != cols:
            scale_b = jnp.where(
                lax.broadcasted_iota(jnp.int32, (1, cols_pad), 1) < cols, scale_b, 1.0
            )
        b_vec[...] = scale_b

    row_out[...] = f_vec[...] * LN2 + jnp.log(a_vec[...])
    col_out[...] = g_vec[...] * LN2 + jnp.log(b_vec[...])


def shards(first_acts, second_acts):
    rows, cols = first_acts.shape[1], second_acts.shape[1]
    n_row, n_col = lax.axis_size("row"), lax.axis_size("col")
    samples = second_acts.shape[0] * n_row
    rows_pad, cols_pad = round_up(rows, LANES), round_up(cols, LANES)
    first = jnp.pad(first_acts, ((0, 0), (0, rows_pad - rows)))
    second = jnp.pad(second_acts, ((0, 0), (0, cols_pad - cols)))
    tile = 512
    remote = (
        first.shape[0] % LANES == 0
        and n_row % 2 == 0
        and n_col % 2 == 0
        and rows_pad >= tile
    )
    if remote:
        a_in, b_in = first.T[None], second
        chunks = n_col
        gathered = (n_col, rows_pad, first.shape[0])
    else:
        b_in = lax.all_gather(second, "row", axis=0, tiled=True)
        a_in = lax.all_gather(first, "col", axis=0, tiled=True).T[None]
        chunks = 1
        gathered = (1, 16, LANES)
    tiles = -(-rows_pad // tile)
    rest = ITERS - 1
    f32 = jnp.float32
    vmem = pltpu.VMEM
    dma = pltpu.SemaphoreType.DMA
    row_out, col_out, unused = pl.pallas_call(
        functools.partial(kernel, rows, cols, rows * n_row, samples, tile, remote),
        out_shape=(
            jax.ShapeDtypeStruct((1, rows_pad), f32),
            jax.ShapeDtypeStruct((1, cols_pad), f32),
            jax.ShapeDtypeStruct(gathered, jnp.bfloat16),
        ),
        in_specs=[pl.BlockSpec(memory_space=pl.ANY)] * 2,
        out_specs=(pl.BlockSpec(memory_space=vmem),) * 2
        + (pl.BlockSpec(memory_space=pl.ANY),),
        scratch_shapes=[
            vmem((samples, cols_pad), jnp.bfloat16),
            vmem((rows_pad, cols_pad), f32),
            vmem((tile, samples), jnp.bfloat16),
            vmem((1, rows_pad), f32),
            vmem((1, cols_pad), f32),
            vmem((1, rows_pad), f32),
            vmem((1, cols_pad), f32),
            vmem((1, cols_pad), f32),
            vmem((8, cols_pad), f32),
            vmem((8, cols_pad), f32),
            vmem((2, rows_pad), f32),
            vmem((n_col - 1, 2, rows_pad), f32),
            vmem((rest, 1, rows_pad), f32),
            vmem((rest, n_col - 1, 1, rows_pad), f32),
            vmem((2, cols_pad), f32),
            vmem((n_row - 1, 2, cols_pad), f32),
            vmem((rest, 1, cols_pad), f32),
            vmem((rest, n_row - 1, 1, cols_pad), f32),
            dma((chunks,)),
            dma((n_col - 1,)),
            dma((n_col - 1,)),
            dma((rest, n_col - 1)),
            dma((rest, n_col - 1)),
            dma((n_row - 1,)),
            dma((n_row - 1,)),
            dma((rest, n_row - 1)),
            dma((rest, n_row - 1)),
            dma,
            dma((tiles, n_col)),
            dma((tiles, n_col)),
            dma((n_row,)),
            dma((n_row,)),
        ],
        compiler_params=pltpu.CompilerParams(
            collective_id=0, has_side_effects=True, vmem_limit_bytes=67043328
        ),
    )(a_in, b_in)
    return row_out[0, :rows], col_out[0, :cols]


def solution(mesh):
    return jax.shard_map(
        shards,
        mesh=mesh,
        in_specs=(P("col", "row"), P("row", "col")),
        out_specs=(P("row"), P("col")),
        check_vma=False,
    )
```
